256 devices in a mesh: tok: 64 (over y, z, core), head: 4 (over x).
Axes of the slice: x: 4, y: 4, z: 8, core: 2. Of those that a mesh axis runs over, the one named last changes fastest.
Arguments:
- latents: float32 [512, 4096], P(None, 'tok'), may hold values from -6 to 6
- doc_keys: bfloat16 [16384, 4096], P('tok', 'head'), may hold values from -500 to 500
- doc_values: bfloat16 [16384, 4096], P('tok', 'head'), may hold values from -6 to 6
- token_mask: int32 [16384], P('tok'), may hold values from 0 to 1, as said below
- shard_lengths: int32 [64], P('tok'), may hold values from 64 to 256, as said below
- query_weight: bfloat16 [4096, 4096], P('tok', 'head'), may hold values from -0.375 to 0.375
- output_weight: bfloat16 [4096, 4096], P('head', 'tok'), may hold values from -0.375 to 0.375
- attn_gain: float32 [4096], P('tok'), may hold values from 0.1 to 1.9
- up_weight: bfloat16 [4096, 4096], P('tok', 'head'), may hold values from -0.1875 to 0.1875
- down_weight: bfloat16 [4096, 4096], P('head', 'tok'), may hold values from -0.1875 to 0.1875
- mlp_gain: float32 [4096], P('tok'), may hold values from 0.1 to 1.9
Outputs:
- encoded: float32 [512, 4096], P(None, 'tok')
The draws below stay inside these ranges and needn't reach their ends.
Inputs may be any that keep to these rules, and one draw needn't show every extreme that they name: `token_mask`: the first token of every aligned block of 256 tokens is 1. Entry j bounds the valid tokens of block j to its first shard_lengths[j]; some entry equals 256.
All inputs are finite; a program needn't handle non-finite values.
Results may differ from the reference program's by a relative error of at most 0.0035.
The reference program's roundings to bfloat16 on the way count: a program that leaves them out, or rounds other values in their place, can miss the bound.
Values may be sent and summed in bfloat16 or wider, within the bound.
No kernel may reach another device: no remote copies, remote signals or barrier semaphores. Data moves between devices by JAX's collectives and lax.ppermute only.
A program may use at most 64 MiB of HBM per device.

```python
import jax
import jax.numpy as jnp
from jax import lax

D = 4096
H = 32
HS = 128
L = 512
FF = 4096
ITERS = 1
TOK_DEV = 256
HD = 4096
TOKENS = 16384
N_TOK = 64


def draw_token_mask(key, part):
    quarter_draw = jax.random.randint(key, (TOKENS,), 0, 4)
    leading = jnp.arange(TOKENS) % TOK_DEV == 0
    return jnp.where(leading | (quarter_draw != 0), 1, 0).astype(jnp.int32)


def draw_shard_lengths(key, part):
    lengths_drawn = jax.random.randint(key, (N_TOK,), TOK_DEV // 4, TOK_DEV + 1)
    full_shard = jax.random.randint(jax.random.fold_in(key, 7), (), 0, N_TOK)
    return jnp.where(jnp.arange(N_TOK) == full_shard, TOK_DEV, lengths_drawn).astype(jnp.int32)


def draw_doc_keys(key, part):
    basic_draw = jax.random.truncated_normal(key, -6.0, 6.0, (TOKENS, HD), jnp.float32)
    return basic_draw.astype(jnp.bfloat16)


def block_scale(rng, shape, pieces, least, top_value):
    level = 1.0
    for axis_at, blocks in pieces:
        draws = jax.random.uniform(jax.random.fold_in(jax.random.fold_in(rng, 6), axis_at), (blocks,), jnp.float32, least / len(pieces), top_value / len(pieces))
        level = level * jnp.repeat(jnp.exp(draws), shape[axis_at] // blocks).reshape((-1,) + (1,) * (len(shape) - 1 - axis_at))
    return level


def normal_values(stream_key, dims, width, bound, cuts=(), held_as=jnp.bfloat16):
    drawn = width * jax.random.normal(stream_key, dims, jnp.float32)
    if cuts:
        drawn = drawn * block_scale(stream_key, dims, cuts, -0.22, 0.18)
    return jnp.clip(drawn, -bound, bound).astype(held_as)


def setup_inputs(seed: int = 0) -> dict:
    keys = jax.random.split(jax.random.key(seed), 12)
    return {
        "latents": normal_values(keys[0], (L, D), 1.0, 6.0, ((1, 64),), jnp.float32),
        "doc_keys": draw_doc_keys(jax.random.fold_in(keys[11], 71), 0),
        "doc_values": normal_values(keys[2], (TOKENS, HD), 1.0, 6.0, ((0, 64), (1, 4))),
        "token_mask": draw_token_mask(jax.random.fold_in(keys[11], 71), 0),
        "shard_lengths": draw_shard_lengths(jax.random.fold_in(keys[11], 71), 0),
        "query_weight": normal_values(keys[5], (D, HD), (D // 16) ** -0.5, 0.375, ((0, 64), (1, 4))),
        "output_weight": normal_values(keys[6], (HD, D), (HD // 16) ** -0.5, 0.375, ((0, 4), (1, 64))),
        "attn_gain": jnp.clip(1.0 + 0.18 * jax.random.normal(keys[7], (D,), jnp.float32), 0.1, 1.9),
        "up_weight": normal_values(keys[8], (D, FF), (D // 4) ** -0.5, 0.1875, ((0, 64), (1, 4))),
        "down_weight": normal_values(keys[9], (FF, D), (FF // 4) ** -0.5, 0.1875, ((0, 4), (1, 64))),
        "mlp_gain": jnp.clip(1.0 + 0.18 * jax.random.normal(keys[10], (D,), jnp.float32), 0.1, 1.9),
    }


epsilon = 1e-05
masked_score = -1e+30

def projected(state, gain, weight):
    scaled = (state * gain).astype(jnp.bfloat16)
    squares = lax.optimization_barrier(jnp.sum(state * state, axis=1))
    inverse = lax.rsqrt(squares / D + epsilon)
    return jnp.dot(scaled, weight, preferred_element_type=jnp.float32) * inverse[:, None]

def combine(left_part, right_part):
    left_top, left_total, left_sum = left_part
    right_top, right_total, right_sum = right_part
    ceiling = jnp.maximum(left_top, right_top)
    left_factor = jnp.exp(left_top - ceiling)
    right_factor = jnp.exp(right_top - ceiling)
    total = left_total * left_factor + right_total * right_factor
    summed = left_sum * left_factor[:, :, None] + right_sum * right_factor[:, :, None]
    return (ceiling, total, summed)

def reference(latents, doc_keys, doc_values, token_mask, shard_lengths, query_weight, output_weight, attn_gain, up_weight, down_weight, mlp_gain):
    score_scale = HS ** (-0.5)
    positions = jnp.arange(TOK_DEV, dtype=jnp.int32)
    valid = (token_mask.reshape(N_TOK, TOK_DEV) == 1) & (positions[None, :] < shard_lengths[:, None])
    key_blocks = doc_keys.reshape(N_TOK, TOK_DEV, H, HS)
    value_blocks = doc_values.reshape(N_TOK, TOK_DEV, H, HS)
    state = latents
    for iteration in range(ITERS):
        queries = projected(state, attn_gain, query_weight).astype(jnp.bfloat16)
        query_heads = queries.reshape(L, H, HS).astype(jnp.float32)

        def shard_step(carry, block):
            key_block, value_block, valid_block = block
            scores = jnp.einsum('lhd,thd->lht', query_heads, key_block.astype(jnp.float32)) * score_scale
            scores = jnp.where(valid_block[None, None, :], scores, masked_score)
            highest = lax.optimization_barrier(jnp.max(scores, axis=2))
            weights = jnp.exp(scores - highest[:, :, None])
            total = lax.optimization_barrier(jnp.sum(weights, axis=2))
            weighted = jnp.einsum('lht,thd->lhd', weights.astype(jnp.bfloat16).astype(jnp.float32), value_block.astype(jnp.float32))
            return (combine(carry, (highest, total, weighted)), None)
        start = (jnp.full((L, H), masked_score, jnp.float32), jnp.zeros((L, H), jnp.float32), jnp.zeros((L, H, HS), jnp.float32))
        merged, unused = lax.scan(shard_step, start, (key_blocks, value_blocks, valid))
        attended = (merged[2] / merged[1][:, :, None]).astype(jnp.bfloat16).reshape(L, HD)
        state = state + jnp.dot(attended, output_weight, preferred_element_type=jnp.float32)
    hidden = jax.nn.gelu(projected(state, mlp_gain, up_weight)).astype(jnp.bfloat16)
    return state + jnp.dot(hidden, down_weight, preferred_element_type=jnp.float32)
```

```python
import jax
import jax.numpy as jnp
from jax import lax
from jax.experimental import pallas as pl
from jax.experimental.pallas import tpu as pltpu
from jax.sharding import Mesh
from jax.sharding import PartitionSpec as P

D = 4096
HS = 128
L = 512
Z = 8
G = 8
BLOCK = 256
TOK = ("y", "z", "c")
YC = ("y", "c")
RING = (0, -1, -2, -3, -4, 1, 2, 3)
epsilon = 1e-05
masked_score = -1e30
f32 = jnp.float32
bf16 = jnp.bfloat16


def vmem(count):
    return [pl.BlockSpec(memory_space=pltpu.VMEM)] * count


def smem():
    return pl.BlockSpec(memory_space=pltpu.SMEM)


def call(kernel, out, name, flops, operands, scalars=0, scratch=()):
    single = not isinstance(out, (list, tuple))
    outs = [out] if single else list(out)
    moved = sum(a.size * a.dtype.itemsize for a in list(operands) + outs)
    result = pl.pallas_call(
        kernel,
        out_shape=outs,
        in_specs=[smem()] * scalars + vmem(len(operands) - scalars),
        out_specs=vmem(len(outs)),
        scratch_shapes=list(scratch),
        name=name,
        cost_estimate=pl.CostEstimate(flops=flops, bytes_accessed=moved, transcendentals=0),
    )(*operands)
    return result[0] if single else result


def shape(dims, dtype):
    return jax.ShapeDtypeStruct(dims, dtype)


def exchange(chunks, axis):
    return lax.all_to_all(chunks, axis, 0, 0, tiled=True)


def thirds(row):
    high = row.astype(bf16)
    rest = row - high.astype(f32)
    middle = rest.astype(bf16)
    return high, middle, (rest - middle.astype(f32)).astype(bf16)


def pack_projection(lat_ref, gain_ref, weight_ref, out_ref):
    turned = lat_ref[...].T
    gain = jnp.broadcast_to(gain_ref[...], (128, 64)).T[:, :1]
    scaled = (turned * gain).astype(bf16)
    squares = jnp.sum(turned * turned, axis=0, keepdims=True)
    high = squares.astype(bf16).astype(f32)
    rest = squares - high
    middle = rest.astype(bf16).astype(f32)
    low = rest - middle
    row = lax.broadcasted_iota(jnp.int32, (16, L), 0)
    tail = jnp.where(row == 0, high, jnp.where(row == 1, middle, jnp.where(row == 2, low, 0.0)))
    tail = tail.astype(bf16)
    for g in range(G):
        out_ref[g, :64, :] = scaled
        out_ref[g, 64:80, :] = tail
        for k in range(4):
            out_ref[g, 80:96, k * 128 : (k + 1) * 128] = weight_ref[
                k * 16 : (k + 1) * 16, g * 128 : (g + 1) * 128
            ]


def project_part(got_ref, lat_ref, gain_ref, out_ref):
    stacked = jnp.concatenate([got_ref[g, :64, :] for g in range(G)], axis=0)
    weight = jnp.concatenate(
        [got_ref[g, 80:96, k * 128 : (k + 1) * 128] for g in range(G) for k in range(4)], axis=0
    )
    turned = lax.dot_general(
        weight, stacked, (((0,), (0,)), ((), ())), preferred_element_type=f32
    )
    squares = jnp.zeros((1, L), f32)
    for g in range(G):
        squares = squares + jnp.sum(got_ref[g, 64:80, :].astype(f32), axis=0, keepdims=True)
    for z in range(Z):
        for k in range(4):
            lanes = slice(k * 128, (k + 1) * 128)
            out_ref[z, k * 16 : (k + 1) * 16, :] = turned[z * 16 : (z + 1) * 16, lanes]
            out_ref[z, 64 + k : 65 + k, :] = squares[:, lanes]
        out_ref[z, 68:72, :64] = jnp.broadcast_to(gain_ref[...], (4, 64))
        out_ref[z, 68:72, 64:] = jnp.zeros((4, 64), f32)
        out_ref[z, 72:104, :64] = lat_ref[z * 64 : z * 64 + 32, :]
        out_ref[z, 72:104, 64:] = lat_ref[z * 64 + 32 : z * 64 + 64, :]


def finish_queries(got_ref, out_ref):
    summed = got_ref[0, :72, :]
    for z in range(1, Z):
        summed = summed + got_ref[z, :72, :]
    for k in range(4):
        inverse = lax.rsqrt(summed[64 + k : 65 + k, :] / D + epsilon)
        queries = (summed[k * 16 : (k + 1) * 16, :] * inverse).astype(bf16)
        for z in range(Z):
            out_ref[z, :, k * 128 : (k + 1) * 128] = queries


def pack_document(length_ref, keys_ref, values_ref, mask_ref, out_ref):
    row = lax.broadcasted_iota(jnp.int32, (2, 128), 0)
    lane = lax.broadcasted_iota(jnp.int32, (2, 128), 1)
    valid = (mask_ref[...] == 1) & (row * 128 + lane < length_ref[0])
    tile = jnp.concatenate([jnp.where(valid, 1.0, 0.0), jnp.zeros((14, 128), f32)], axis=0)
    tile = tile.astype(bf16)
    for g in range(G):
        lanes = slice(g * 128, (g + 1) * 128)
        out_ref[g, :BLOCK, :] = keys_ref[:, lanes]
        out_ref[g, BLOCK : 2 * BLOCK, :] = values_ref[:, lanes]
        out_ref[g, 2 * BLOCK :, :] = tile


def attend(got_ref, doc_ref, out_ref, top_ref, total_ref, sum_ref):
    queries = jnp.concatenate([got_ref[z] for z in range(Z)], axis=0)
    top_ref[...] = jnp.full((8, L), masked_score, f32)
    total_ref[...] = jnp.zeros((8, L), f32)
    sum_ref[...] = jnp.zeros((HS, L), f32)

    def one_block(b, carry):
        keys = doc_ref[b, :BLOCK, :]
        values = doc_ref[b, BLOCK : 2 * BLOCK, :]
        mask = doc_ref[b, 2 * BLOCK :, :].astype(f32)
        flags = jnp.concatenate([mask[0:8, :].T[:, :1], mask[0:8, :].T[:, 1:2]], axis=0)
        scores = jnp.dot(keys, queries, preferred_element_type=f32) * HS ** (-0.5)
        scores = jnp.where(flags > 0.5, scores, masked_score)
        highest = jnp.max(scores, axis=0, keepdims=True)
        weights = jnp.exp(scores - highest)
        total = jnp.sum(weights, axis=0, keepdims=True)
        weighted = lax.dot_general(
            values, weights.astype(bf16), (((0,), (0,)), ((), ())), preferred_element_type=f32
        )
        before = top_ref[0:1, :]
        ceiling = jnp.maximum(before, highest)
        old = jnp.exp(before - ceiling)
        new = jnp.exp(highest - ceiling)
        top_ref[0:1, :] = ceiling
        total_ref[0:1, :] = total_ref[0:1, :] * old + total * new
        sum_ref[...] = sum_ref[...] * old + weighted * new
        return carry

    lax.fori_loop(0, G, one_block, 0)
    lane = lax.broadcasted_iota(jnp.int32, (1, 128), 1)
    for k in range(4):
        lanes = slice(k * 128, (k + 1) * 128)

        def fold(first, second, z):
            first, second = (
                (first, pltpu.roll(second, 64, 1)) if z == 0 else (pltpu.roll(first, 64, 1), second)
            )
            return jnp.where(lane < 64, first, second)

        upper = sum_ref[:64, lanes]
        lower = sum_ref[64:, lanes]
        top = top_ref[:, lanes]
        total = total_ref[:, lanes]
        row = lax.broadcasted_iota(jnp.int32, (8, 128), 0)
        for z in range(2):
            out_ref[2 * k + z, :64, :] = fold(upper, lower, z)
            tops = fold(top, top, z)
            totals = fold(total, total, z)
            out_ref[2 * k + z, 64:72, :] = jnp.where(
                row == 0, tops, jnp.where(row == 1, pltpu.roll(totals, 1, 0), 0.0)
            )


def join_blocks(got_ref, out_ref):
    ceiling = got_ref[0, 64:65, :]
    for z in range(1, Z):
        ceiling = jnp.maximum(ceiling, got_ref[z, 64:65, :])
    total = jnp.zeros((1, 128), f32)
    summed = jnp.zeros((64, 128), f32)
    for z in range(Z):
        factor = jnp.exp(got_ref[z, 64:65, :] - ceiling)
        total = total + got_ref[z, 65:66, :] * factor
        summed = summed + got_ref[z, :64, :] * factor
    folded = (summed / total).T
    attended = jnp.concatenate([folded[:64, :], folded[64:, :]], axis=1).astype(bf16)
    for g in range(G):
        out_ref[g] = attended


def turn_weights(output_ref, up_ref, down_ref, out_ref):
    out_ref[:64, :] = output_ref[...].T
    out_ref[64:128, :] = up_ref[...]
    out_ref[128:, :] = down_ref[...].T


def output_part(got_ref, *refs):
    weights, out_ref = refs[:Z], refs[Z]
    attended = jnp.concatenate([got_ref[g] for g in range(G)], axis=1)
    for k in range(4):
        pair = jnp.concatenate([weights[2 * k][:64, :], weights[2 * k + 1][:64, :]], axis=0)
        out_ref[:, k * 128 : (k + 1) * 128] = lax.dot_general(
            attended, pair, (((1,), (1,)), ((), ())), preferred_element_type=f32
        )


def up_part(place_ref, first_ref, a_ref, b_ref, c_ref, d_ref, *refs):
    weights, out_ref, state_ref = refs[:Z], refs[Z], refs[Z + 1]
    update = (a_ref[...] + b_ref[...]) + (c_ref[...] + d_ref[...])
    states, gains = [], []
    for j, offset in enumerate(RING):
        z = lax.rem(place_ref[0] + offset + Z, Z)
        piece = first_ref[z, 72:104, :]
        states.append(jnp.concatenate([piece[:, :64], piece[:, 64:]], axis=0))
        gains.append(first_ref[z, 68:69, :][:, :64])
    state = jnp.concatenate(states, axis=1) + update
    gain = jnp.concatenate(gains, axis=1)
    state_ref[...] = state
    squares = jnp.sum(state * state, axis=1, keepdims=True)
    scaled = (state * gain).astype(bf16)
    weight = jnp.concatenate([w[64:128, :] for w in weights], axis=0)
    summed = jnp.dot(scaled, weight, preferred_element_type=f32)
    for g in range(G):
        rows = slice(g * 8, (g + 1) * 8)
        out_ref[g, :, :1024] = summed[rows, :]
        out_ref[g, :, 1024:] = jnp.broadcast_to(squares[rows, :], (8, 128))


def finish_hidden(got_ref, out_ref):
    summed = got_ref[0]
    for g in range(1, G):
        summed = summed + got_ref[g]
    inverse = lax.rsqrt(summed[:, 1024:1025] / D + epsilon)
    hidden = jax.nn.gelu(summed[:, :1024] * inverse).astype(bf16)
    for g in range(G):
        out_ref[g] = hidden


def down_part(got_ref, *refs):
    weights, out_ref = refs[:Z], refs[Z]
    hidden = jnp.concatenate([got_ref[g].astype(f32) for g in range(G)], axis=0).astype(bf16)
    for k in range(4):
        pair = jnp.concatenate([weights[2 * k][128:, :], weights[2 * k + 1][128:, :]], axis=0)
        out_ref[:, k * 128 : (k + 1) * 128] = lax.dot_general(
            hidden, pair, (((1,), (1,)), ((), ())), preferred_element_type=f32
        )


def pack_encoded(place_ref, state_ref, a_ref, b_ref, c_ref, d_ref, out_ref):
    encoded = state_ref[...] + ((a_ref[...] + b_ref[...]) + (c_ref[...] + d_ref[...]))
    for j, offset in enumerate(RING):
        z = lax.rem(place_ref[0] + offset + Z, Z)
        piece = encoded[:, j * 64 : (j + 1) * 64]
        out_ref[z] = jnp.concatenate([piece[:32, :], piece[32:, :]], axis=1)


def unpack_encoded(got_ref, out_ref):
    for z in range(Z):
        out_ref[z * 64 : z * 64 + 32, :] = got_ref[z, :, :64]
        out_ref[z * 64 + 32 : z * 64 + 64, :] = got_ref[z, :, 64:]


def shifted(array, axis, step):
    count = lax.axis_size(axis)
    return lax.ppermute(array, axis, [(i, (i + step) % count) for i in range(count)])


def paired(array, axis, flip):
    return lax.ppermute(array, axis, [(i, i ^ flip) for i in range(lax.axis_size(axis))])


def around_ring(array):
    forward, backward = [array], [array]
    for k in range(4):
        forward.append(shifted(forward[-1], "z", 1))
        if k < 3:
            backward.append(shifted(backward[-1], "z", -1))
    return forward + backward[1:]


def shards(
    latents,
    doc_keys,
    doc_values,
    token_mask,
    shard_lengths,
    query_weight,
    output_weight,
    attn_gain,
    up_weight,
    down_weight,
    mlp_gain,
):
    place = lax.axis_index("z").astype(jnp.int32)[None]
    attn_gain = attn_gain.reshape(1, 64)
    mlp_gain = mlp_gain.reshape(1, 64)

    packed = call(
        pack_projection,
        shape((G, 96, L), bf16),
        "pack_projection",
        4_000_000,
        (latents, attn_gain, query_weight),
    )
    packed = exchange(packed, YC)
    document = call(
        pack_document,
        shape((G, 2 * BLOCK + 16, HS), bf16),
        "pack_document",
        4_000_000,
        (shard_lengths, doc_keys, doc_values, token_mask.reshape(2, 128)),
        scalars=1,
    )
    document = exchange(document, YC)
    turned = call(
        turn_weights,
        shape((192, 1024), bf16),
        "turn_weights",
        4_000_000,
        (output_weight, up_weight, down_weight),
    )
    weights = around_ring(turned)

    part = call(
        project_part,
        shape((Z, 104, 128), f32),
        "project_part",
        70_000_000,
        (packed, latents, mlp_gain),
    )
    first = exchange(part, "z")
    queries = call(
        finish_queries, shape((Z, 16, L), bf16), "finish_queries", 1_000_000, (first,)
    )
    queries = exchange(queries, "z")
    blocks = call(
        attend,
        shape((Z, 72, 128), f32),
        "attend",
        540_000_000,
        (queries, document),
        scratch=(
            pltpu.VMEM((8, L), f32),
            pltpu.VMEM((8, L), f32),
            pltpu.VMEM((HS, L), f32),
        ),
    )
    blocks = exchange(blocks, "z")
    attended = call(join_blocks, shape((G, 64, 128), bf16), "join_blocks", 1_000_000, (blocks,))
    attended = exchange(attended, YC)
    part = call(
        output_part, shape((64, 512), f32), "output_part", 70_000_000, (attended, *weights)
    )
    parts = [part] + [paired(part, "x", flip) for flip in (1, 2, 3)]
    summed, state = call(
        up_part,
        (shape((G, 8, 1152), f32), shape((64, 512), f32)),
        "up_part",
        70_000_000,
        (place, first, *parts, *weights),
        scalars=1,
    )
    summed = exchange(summed, YC)
    hidden = call(finish_hidden, shape((G, 8, 1024), bf16), "finish_hidden", 1_000_000, (summed,))
    hidden = exchange(hidden, YC)
    part = call(down_part, shape((64, 512), f32), "down_part", 70_000_000, (hidden, *weights))
    parts = [part] + [paired(part, "x", flip) for flip in (1, 2, 3)]
    encoded = call(
        pack_encoded,
        shape((Z, 32, 128), f32),
        "pack_encoded",
        1_000_000,
        (place, state, *parts),
        scalars=1,
    )
    encoded = exchange(encoded, "z")
    return call(unpack_encoded, shape((L, 64), f32), "unpack_encoded", 1_000_000, (encoded,))


def solution(mesh):
    split = Mesh(mesh.devices.reshape(4, 8, 2, 4), ("y", "z", "c", "x"))
    return jax.shard_map(
        shards,
        mesh=split,
        in_specs=(
            P(None, TOK),
            P(TOK, "x"),
            P(TOK, "x"),
            P(TOK),
            P(TOK),
            P(TOK, "x"),
            P("x", TOK),
            P(TOK),
            P(TOK, "x"),
            P("x", TOK),
            P(TOK),
        ),
        out_specs=P(None, TOK),
        check_vma=False,
    )
```

```python
import functools

import jax
import jax.numpy as jnp
from jax import lax
from jax.experimental import pallas as pl
from jax.experimental.pallas import tpu as pltpu
from jax.sharding import Mesh
from jax.sharding import PartitionSpec as P

D = 4096
HS = 128
L = 512
Z = 8
G = 8
BLOCK = 256
TOK = ("y", "z", "c")
YC = ("y", "c")
RING = (0, -1, -2, -3, -4, 1, 2, 3)
epsilon = 1e-05
masked_score = -1e30
f32 = jnp.float32
bf16 = jnp.bfloat16


def vmem(count):
    return [pl.BlockSpec(memory_space=pltpu.VMEM)] * count


def smem():
    return pl.BlockSpec(memory_space=pltpu.SMEM)


def call(kernel, out, name, flops, operands, scalars=0, scratch=(), after=()):
    single = not isinstance(out, (list, tuple))
    outs = [out] if single else list(out)
    moved = sum(a.size * a.dtype.itemsize for a in list(operands) + outs)
    result = pl.pallas_call(
        kernel,
        out_shape=outs,
        in_specs=[pl.BlockSpec(memory_space=pl.ANY)] * len(after)
        + [smem()] * scalars
        + vmem(len(operands) - scalars),
        out_specs=vmem(len(outs)),
        scratch_shapes=list(scratch),
        name=name,
        compiler_params=pltpu.CompilerParams(vmem_limit_bytes=12 * 1024 * 1024),
        cost_estimate=pl.CostEstimate(flops=flops, bytes_accessed=moved, transcendentals=0),
    )(*after, *operands)
    return result[0] if single else result


def shape(dims, dtype):
    return jax.ShapeDtypeStruct(dims, dtype)


def exchange(chunks, axis):
    return lax.all_to_all(chunks, axis, 0, 0, tiled=True)


def thirds(row):
    high = row.astype(bf16)
    rest = row - high.astype(f32)
    middle = rest.astype(bf16)
    return high, middle, (rest - middle.astype(f32)).astype(bf16)


def pack_projection(lat_ref, gain_ref, weight_ref, out_ref):
    turned = lat_ref[...]
    gain = jnp.broadcast_to(gain_ref[...], (128, 64)).T[:, :1]
    scaled = (turned * gain).astype(bf16)
    squares = jnp.sum(turned * turned, axis=0, keepdims=True)
    high = squares.astype(bf16).astype(f32)
    rest = squares - high
    middle = rest.astype(bf16).astype(f32)
    low = rest - middle
    row = lax.broadcasted_iota(jnp.int32, (16, L), 0)
    tail = jnp.where(row == 0, high, jnp.where(row == 1, middle, jnp.where(row == 2, low, 0.0)))
    tail = tail.astype(bf16)
    for g in range(G):
        out_ref[g, :64, :] = scaled
        out_ref[g, 64:80, :] = tail
        for k in range(4):
            out_ref[g, 80:96, k * 128 : (k + 1) * 128] = weight_ref[
                k * 16 : (k + 1) * 16, g * 128 : (g + 1) * 128
            ]


def project_part(got_ref, lat_ref, gain_ref, out_ref):
    stacked = jnp.concatenate([got_ref[g, :64, :] for g in range(G)], axis=0)
    weight = jnp.concatenate(
        [got_ref[g, 80:96, k * 128 : (k + 1) * 128] for g in range(G) for k in range(4)], axis=0
    )
    turned = lax.dot_general(
        weight, stacked, (((0,), (0,)), ((), ())), preferred_element_type=f32
    )
    squares = jnp.zeros((1, L), f32)
    for g in range(G):
        squares = squares + jnp.sum(got_ref[g, 64:80, :].astype(f32), axis=0, keepdims=True)
    for z in range(Z):
        for k in range(4):
            lanes = slice(k * 128, (k + 1) * 128)
            out_ref[z, k * 16 : (k + 1) * 16, :] = turned[z * 16 : (z + 1) * 16, lanes]
            out_ref[z, 64 + k : 65 + k, :] = squares[:, lanes]
        out_ref[z, 68:72, :64] = jnp.broadcast_to(gain_ref[...], (4, 64))
        out_ref[z, 68:72, 64:] = jnp.zeros((4, 64), f32)
    lane = lax.broadcasted_iota(jnp.int32, (1, 128), 1)
    for k in range(4):
        lanes = slice(k * 128, (k + 1) * 128)
        upper, lower = lat_ref[:32, lanes], lat_ref[32:, lanes]
        out_ref[2 * k, 72:104, :] = jnp.where(lane < 64, upper, pltpu.roll(lower, 64, 1))
        out_ref[2 * k + 1, 72:104, :] = jnp.where(lane < 64, pltpu.roll(upper, 64, 1), lower)


def place_latents(place_ref, first_ref, state_ref, gain_ref):
    states, gains = [], []
    for offset in RING:
        z = lax.rem(place_ref[0] + offset + Z, Z)
        piece = first_ref[z, 72:104, :].T
        states.append(jnp.concatenate([piece[:64, :], piece[64:, :]], axis=1))
        gains.append(first_ref[z, 68:69, :][:, :64])
    state_ref[...] = jnp.concatenate(states, axis=1)
    gain_ref[...] = jnp.concatenate(gains, axis=1)


def finish_queries(got_ref, out_ref):
    summed = got_ref[0, :72, :]
    for z in range(1, Z):
        summed = summed + got_ref[z, :72, :]
    for k in range(4):
        inverse = lax.rsqrt(summed[64 + k : 65 + k, :] / D + epsilon)
        queries = (summed[k * 16 : (k + 1) * 16, :] * inverse).astype(bf16)
        for z in range(Z):
            out_ref[z, :, k * 128 : (k + 1) * 128] = queries


def pack_document(
    after_ref, length_ref, place_ref, keys_ref, values_ref, mask_ref, own_ref, a_ref, b_ref, c_ref
):
    row = lax.broadcasted_iota(jnp.int32, (2, 128), 0)
    lane = lax.broadcasted_iota(jnp.int32, (2, 128), 1)
    valid = (mask_ref[...] == 1) & (row * 128 + lane < length_ref[0])
    tile = jnp.concatenate([jnp.where(valid, 1.0, 0.0), jnp.zeros((14, 128), f32)], axis=0)
    tile = tile.astype(bf16)
    for flip, out_ref in enumerate((own_ref, a_ref, b_ref, c_ref)):
        for other in range(2):
            head = (place_ref[1] ^ flip) * 2 + (place_ref[2] ^ other)
            lanes = pl.ds(pl.multiple_of(head * HS, HS), HS)
            out_ref[other, :BLOCK, :] = keys_ref[:, lanes]
            out_ref[other, BLOCK : 2 * BLOCK, :] = values_ref[:, lanes]
            out_ref[other, 2 * BLOCK :, :] = tile


def attend(got_ref, near_ref, far_ref, out_ref, top_ref, total_ref, sum_ref):
    queries = jnp.concatenate([got_ref[z] for z in range(Z)], axis=0)
    top_ref[...] = jnp.full((8, L), masked_score, f32)
    total_ref[...] = jnp.zeros((8, L), f32)
    sum_ref[...] = jnp.zeros((HS, L), f32)

    def one_block(doc_ref, b, carry):
        keys = doc_ref[b, :BLOCK, :]
        values = doc_ref[b, BLOCK : 2 * BLOCK, :]
        mask = doc_ref[b, 2 * BLOCK :, :].astype(f32)
        flags = jnp.concatenate([mask[0:8, :].T[:, :1], mask[0:8, :].T[:, 1:2]], axis=0)
        scores = jnp.dot(keys, queries, preferred_element_type=f32) * HS ** (-0.5)
        scores = jnp.where(flags > 0.5, scores, masked_score)
        highest = jnp.max(scores, axis=0, keepdims=True)
        weights = jnp.exp(scores - highest)
        total = jnp.sum(weights, axis=0, keepdims=True)
        weighted = lax.dot_general(
            values, weights.astype(bf16), (((0,), (0,)), ((), ())), preferred_element_type=f32
        )
        before = top_ref[0:1, :]
        ceiling = jnp.maximum(before, highest)
        old = jnp.exp(before - ceiling)
        new = jnp.exp(highest - ceiling)
        top_ref[0:1, :] = ceiling
        total_ref[0:1, :] = total_ref[0:1, :] * old + total * new
        sum_ref[...] = sum_ref[...] * old + weighted * new
        return carry

    lax.fori_loop(0, 4, functools.partial(one_block, near_ref), 0)
    lax.fori_loop(0, 4, functools.partial(one_block, far_ref), 0)
    lane = lax.broadcasted_iota(jnp.int32, (1, 128), 1)
    for k in range(4):
        lanes = slice(k * 128, (k + 1) * 128)

        def fold(first, second, z):
            first, second = (
                (first, pltpu.roll(second, 64, 1)) if z == 0 else (pltpu.roll(first, 64, 1), second)
            )
            return jnp.where(lane < 64, first, second)

        upper = sum_ref[:64, lanes]
        lower = sum_ref[64:, lanes]
        top = top_ref[:, lanes]
        total = total_ref[:, lanes]
        row = lax.broadcasted_iota(jnp.int32, (8, 128), 0)
        for z in range(2):
            out_ref[2 * k + z, :64, :] = fold(upper, lower, z)
            tops = fold(top, top, z)
            totals = fold(total, total, z)
            out_ref[2 * k + z, 64:72, :] = jnp.where(
                row == 0, tops, jnp.where(row == 1, pltpu.roll(totals, 1, 0), 0.0)
            )


def join_blocks(got_ref, out_ref):
    ceiling = got_ref[0, 64:65, :]
    for z in range(1, Z):
        ceiling = jnp.maximum(ceiling, got_ref[z, 64:65, :])
    total = jnp.zeros((1, 128), f32)
    summed = jnp.zeros((64, 128), f32)
    for z in range(Z):
        factor = jnp.exp(got_ref[z, 64:65, :] - ceiling)
        total = total + got_ref[z, 65:66, :] * factor
        summed = summed + got_ref[z, :64, :] * factor
    folded = (summed / total).T
    attended = jnp.concatenate([folded[:64, :], folded[64:, :]], axis=1).astype(bf16)
    for g in range(G):
        out_ref[g] = attended


def output_part(got_ref, *refs):
    weights, out_ref = refs[:Z], refs[Z]
    attended = jnp.concatenate([got_ref[g] for g in range(G)], axis=1)
    for k in range(4):
        pair = jnp.concatenate([weights[2 * k][:64, :], weights[2 * k + 1][:64, :]], axis=0)
        out_ref[:, k * 128 : (k + 1) * 128] = lax.dot_general(
            attended, pair, (((1,), (1,)), ((), ())), preferred_element_type=f32
        )


def up_part(latents_ref, gain_ref, a_ref, b_ref, c_ref, d_ref, *refs):
    weights, out_ref, state_ref = refs[:Z], refs[Z], refs[Z + 1]
    state = latents_ref[...] + ((a_ref[...] + b_ref[...]) + (c_ref[...] + d_ref[...]))
    gain = gain_ref[...]
    state_ref[...] = state
    squares = jnp.sum(state * state, axis=1, keepdims=True)
    scaled = (state * gain).astype(bf16)
    weight = jnp.concatenate([w[64:128, :] for w in weights], axis=0)
    summed = jnp.dot(scaled, weight, preferred_element_type=f32)
    for g in range(G):
        rows = slice(g * 8, (g + 1) * 8)
        out_ref[g, :, :1024] = summed[rows, :]
        out_ref[g, :, 1024:] = jnp.broadcast_to(squares[rows, :], (8, 128))


def finish_hidden(got_ref, out_ref):
    summed = got_ref[0]
    for g in range(1, G):
        summed = summed + got_ref[g]
    inverse = lax.rsqrt(summed[:, 1024:1025] / D + epsilon)
    hidden = jax.nn.gelu(summed[:, :1024] * inverse).astype(bf16)
    for g in range(G):
        out_ref[g] = hidden


def down_part(place_ref, got_ref, state_ref, *refs):
    weights, out_ref = refs[:Z], refs[Z]
    hidden = jnp.concatenate([got_ref[g].astype(f32) for g in range(G)], axis=0).astype(bf16)
    for k in range(4):
        pair = jnp.concatenate([weights[2 * k][128:, :], weights[2 * k + 1][128:, :]], axis=0)
        lanes = slice(k * 128, (k + 1) * 128)
        summed = lax.dot_general(
            hidden, pair, (((1,), (1,)), ((), ())), preferred_element_type=f32
        )
        summed = summed + jnp.where(place_ref[3] == 0, state_ref[:, lanes], 0.0)
        turned = summed.T
        for half in range(2):
            z = lax.rem(place_ref[0] + RING[2 * k + half] + Z, Z)
            piece = turned[half * 64 : half * 64 + 64, :]
            folded = jnp.concatenate([piece[:32, :], piece[32:, :]], axis=1)
            for x in range(4):
                out_ref[z * 4 + x] = folded


def unpack_encoded(got_ref, out_ref):
    lane = lax.broadcasted_iota(jnp.int32, (1, 128), 1)

    def summed(z):
        return (got_ref[4 * z] + got_ref[4 * z + 1]) + (got_ref[4 * z + 2] + got_ref[4 * z + 3])

    for k in range(4):
        lanes = slice(k * 128, (k + 1) * 128)
        first, second = summed(2 * k), summed(2 * k + 1)
        out_ref[:32, lanes] = jnp.where(lane < 64, first, pltpu.roll(second, 64, 1))
        out_ref[32:, lanes] = jnp.where(lane < 64, pltpu.roll(first, 64, 1), second)


def shifted(array, axis, step):
    count = lax.axis_size(axis)
    return lax.ppermute(array, axis, [(i, (i + step) % count) for i in range(count)])


def paired(array, axis, flip):
    return lax.ppermute(array, axis, [(i, i ^ flip) for i in range(lax.axis_size(axis))])


def held_until(array, milestone):
    return lax.optimization_barrier((array, milestone))[0]


def together(*arrays):
    return lax.optimization_barrier(arrays)


def ring_step(forward, backward):
    forward.append(shifted(forward[-1], "z", 1))
    if len(backward) < 4:
        backward.append(shifted(backward[-1], "z", -1))


def shards(
    latents,
    doc_keys,
    doc_values,
    token_mask,
    shard_lengths,
    query_weight,
    output_weight,
    attn_gain,
    up_weight,
    down_weight,
    mlp_gain,
):
    place = jnp.stack([lax.axis_index(name) for name in ("z", "y", "c", "x")]).astype(jnp.int32)
    attn_gain = attn_gain.reshape(1, 64)
    mlp_gain = mlp_gain.reshape(1, 64)
    latents = latents.T

    packed = call(
        pack_projection,
        shape((G, 96, L), bf16),
        "pack_projection",
        4_000_000,
        (latents, attn_gain, query_weight),
    )
    weights = jnp.concatenate([output_weight.T, up_weight, down_weight.T], axis=0)
    forward = [held_until(weights, packed)]
    backward = [forward[0]]
    ring_step(forward, backward)
    piece = shape((2, 2 * BLOCK + 16, HS), bf16)
    pieces = call(
        pack_document,
        (piece,) * 4,
        "pack_document",
        4_000_000,
        (shard_lengths, place, doc_keys, doc_values, token_mask.reshape(2, 128)),
        scalars=2,
        after=(packed,),
    )
    packed = exchange(packed, YC)
    packed, forward[-1], backward[-1], *pieces = together(
        packed, forward[-1], backward[-1], *pieces
    )
    part = call(
        project_part,
        shape((Z, 104, 128), f32),
        "project_part",
        70_000_000,
        (packed, latents, mlp_gain),
    )
    first = exchange(part, "z")
    *pieces, _ = together(*pieces, part)
    pieces = [pieces[0]] + [paired(pieces[flip], "y", flip) for flip in (1, 2, 3)]
    ring_step(forward, backward)
    first, forward[-1], backward[-1] = together(first, forward[-1], backward[-1])
    queries = call(
        finish_queries, shape((Z, 16, L), bf16), "finish_queries", 1_000_000, (first,)
    )
    far = paired(jnp.stack([p[1] for p in pieces]), "c", 1)
    near = jnp.stack([p[0] for p in pieces])
    ring_step(forward, backward)
    queries = exchange(queries, "z")
    latent_rows, gain_row = call(
        place_latents,
        (shape((64, 512), f32), shape((1, 512), f32)),
        "place_latents",
        1_000_000,
        (place, first),
        scalars=1,
    )
    blocks = call(
        attend,
        shape((Z, 72, 128), f32),
        "attend",
        540_000_000,
        (queries, near, far),
        scratch=(
            pltpu.VMEM((8, L), f32),
            pltpu.VMEM((8, L), f32),
            pltpu.VMEM((HS, L), f32),
        ),
    )
    blocks, forward[-1], backward[-1] = together(blocks, forward[-1], backward[-1])
    ring_step(forward, backward)
    blocks = exchange(blocks, "z")
    blocks, forward[-1] = together(blocks, forward[-1])
    weights = forward + backward[1:]
    attended = call(join_blocks, shape((G, 64, 128), bf16), "join_blocks", 1_000_000, (blocks,))
    attended = exchange(attended, YC)
    part = call(
        output_part,
        shape((64, 512), f32),
        "output_part",
        70_000_000,
        (attended, *weights),
    )
    parts = [part] + [paired(part, "x", flip) for flip in (1, 2, 3)]
    summed, state = call(
        up_part,
        (shape((G, 8, 1152), f32), shape((64, 512), f32)),
        "up_part",
        70_000_000,
        (latent_rows, gain_row, *parts, *weights),
    )
    summed = exchange(summed, YC)
    hidden = call(finish_hidden, shape((G, 8, 1024), bf16), "finish_hidden", 1_000_000, (summed,))
    hidden = exchange(hidden, YC)
    encoded = call(
        down_part,
        shape((32, 32, 128), f32),
        "down_part",
        70_000_000,
        (place, hidden, state, *weights),
        scalars=1,
    )
    encoded = exchange(encoded, ("z", "x"))
    return call(unpack_encoded, shape((64, L), f32), "unpack_encoded", 1_000_000, (encoded,)).T


def solution(mesh):
    split = Mesh(mesh.devices.reshape(4, 8, 2, 4), ("y", "z", "c", "x"))
    return jax.shard_map(
        shards,
        mesh=split,
        in_specs=(
            P(None, TOK),
            P(TOK, "x"),
            P(TOK, "x"),
            P(TOK),
            P(TOK),
            P(TOK, "x"),
            P("x", TOK),
            P(TOK),
            P(TOK, "x"),
            P("x", TOK),
            P(TOK),
        ),
        out_specs=P(None, TOK),
        check_vma=False,
    )
```

```python
import functools

import jax
import jax.numpy as jnp
from jax import lax
from jax.experimental import pallas as pl
from jax.experimental.pallas import tpu as pltpu
from jax.sharding import Mesh
from jax.sharding import PartitionSpec as P

D = 4096
HS = 128
L = 512
Z = 8
G = 8
BLOCK = 256
TOK = ("y", "z", "c")
YC = ("y", "c")
RING = (0, -1, -2, -3, -4, 1, 2, 3)
epsilon = 1e-05
masked_score = -1e30
f32 = jnp.float32
bf16 = jnp.bfloat16


def vmem(count):
    return [pl.BlockSpec(memory_space=pltpu.VMEM)] * count


def smem():
    return pl.BlockSpec(memory_space=pltpu.SMEM)


def call(kernel, out, flops, operands, scalars=0, scratch=(), after=()):
    single = not isinstance(out, (list, tuple))
    outs = [out] if single else list(out)
    moved = sum(a.size * a.dtype.itemsize for a in list(operands) + outs)
    result = pl.pallas_call(
        kernel,
        out_shape=outs,
        in_specs=[pl.BlockSpec(memory_space=pl.ANY)] * len(after)
        + [smem()] * scalars
        + vmem(len(operands) - scalars),
        out_specs=vmem(len(outs)),
        scratch_shapes=list(scratch),
        compiler_params=pltpu.CompilerParams(vmem_limit_bytes=12 * 1024 * 1024),
        cost_estimate=pl.CostEstimate(flops=flops, bytes_accessed=moved, transcendentals=0),
    )(*after, *operands)
    return result[0] if single else result


def shape(dims, dtype):
    return jax.ShapeDtypeStruct(dims, dtype)


def exchange(chunks, axis):
    return lax.all_to_all(chunks, axis, 0, 0, tiled=True)


def pack_projection(place_ref, lat_ref, gain_ref, weight_ref, own_ref, a_ref, b_ref, c_ref):
    turned = lat_ref[...]
    gain = jnp.broadcast_to(gain_ref[...], (128, 64)).T[:, :1]
    scaled = (turned * gain).astype(bf16)
    squares = jnp.sum(turned * turned, axis=0, keepdims=True)
    high = squares.astype(bf16).astype(f32)
    rest = squares - high
    middle = rest.astype(bf16).astype(f32)
    low = rest - middle
    row = lax.broadcasted_iota(jnp.int32, (16, L), 0)
    tail = jnp.where(row == 0, high, jnp.where(row == 1, middle, jnp.where(row == 2, low, 0.0)))
    tail = tail.astype(bf16)
    for flip, out_ref in enumerate((own_ref, a_ref, b_ref, c_ref)):
        out_ref[16:80, :] = scaled
        out_ref[80:96, :] = tail
        for other, at in ((0, 0), (1, 96)):
            head = (place_ref[1] ^ flip) * 2 + (place_ref[2] ^ other)
            lanes = pl.ds(pl.multiple_of(head * HS, HS), HS)
            for k in range(4):
                out_ref[at : at + 16, k * 128 : (k + 1) * 128] = weight_ref[
                    k * 16 : (k + 1) * 16, lanes
                ]


def project_part(*refs):
    got, (lat_ref, gain_ref, out_ref) = refs[:8], refs[8:]
    stacked = jnp.concatenate([ref[16:80, :] for ref in got], axis=0)
    weight = jnp.concatenate(
        [
            ref[at : at + 16, k * 128 : (k + 1) * 128]
            for ref, at in zip(got, (0,) * 4 + (96,) * 4)
            for k in range(4)
        ],
        axis=0,
    )
    turned = lax.dot_general(
        weight, stacked, (((0,), (0,)), ((), ())), preferred_element_type=f32
    )
    squares = jnp.zeros((1, L), f32)
    for ref in got:
        squares = squares + jnp.sum(ref[80:96, :].astype(f32), axis=0, keepdims=True)
    for z in range(Z):
        for k in range(4):
            lanes = slice(k * 128, (k + 1) * 128)
            out_ref[z, k * 16 : (k + 1) * 16, :] = turned[z * 16 : (z + 1) * 16, lanes]
            out_ref[z, 64 + k : 65 + k, :] = squares[:, lanes]
        out_ref[z, 68:72, :64] = jnp.broadcast_to(gain_ref[...], (4, 64))
        out_ref[z, 68:72, 64:] = jnp.zeros((4, 64), f32)
    lane = lax.broadcasted_iota(jnp.int32, (1, 128), 1)
    for k in range(4):
        lanes = slice(k * 128, (k + 1) * 128)
        upper, lower = lat_ref[:32, lanes], lat_ref[32:, lanes]
        out_ref[2 * k, 72:104, :] = jnp.where(lane < 64, upper, pltpu.roll(lower, 64, 1))
        out_ref[2 * k + 1, 72:104, :] = jnp.where(lane < 64, pltpu.roll(upper, 64, 1), lower)


def place_latents(place_ref, first_ref, state_ref, gain_ref):
    states, gains = [], []
    for offset in RING:
        z = lax.rem(place_ref[0] + offset + Z, Z)
        piece = first_ref[z, 72:104, :].T
        states.append(jnp.concatenate([piece[:64, :], piece[64:, :]], axis=1))
        gains.append(first_ref[z, 68:69, :][:, :64])
    state_ref[...] = jnp.concatenate(states, axis=1)
    gain_ref[...] = jnp.concatenate(gains, axis=1)


def finish_queries(got_ref, out_ref):
    summed = got_ref[0, :72, :]
    for z in range(1, Z):
        summed = summed + got_ref[z, :72, :]
    for k in range(4):
        inverse = lax.rsqrt(summed[64 + k : 65 + k, :] / D + epsilon)
        queries = (summed[k * 16 : (k + 1) * 16, :] * inverse).astype(bf16)
        for z in range(Z):
            out_ref[z, :, k * 128 : (k + 1) * 128] = queries


def pack_document(
    after_ref, length_ref, place_ref, keys_ref, values_ref, mask_ref, near_ref, far_ref
):
    row = lax.broadcasted_iota(jnp.int32, (2, 128), 0)
    lane = lax.broadcasted_iota(jnp.int32, (2, 128), 1)
    valid = (mask_ref[...] == 1) & (row * 128 + lane < length_ref[0])
    tile = jnp.concatenate([jnp.where(valid, 1.0, 0.0), jnp.zeros((14, 128), f32)], axis=0)
    tile = tile.astype(bf16)
    for flip in range(4):
        for other, out_ref in enumerate((near_ref, far_ref)):
            head = (place_ref[1] ^ flip) * 2 + (place_ref[2] ^ other)
            lanes = pl.ds(pl.multiple_of(head * HS, HS), HS)
            out_ref[flip, :BLOCK, :] = keys_ref[:, lanes]
            out_ref[flip, BLOCK : 2 * BLOCK, :] = values_ref[:, lanes]
            out_ref[flip, 2 * BLOCK :, :] = tile


def pair_document(after_ref, near_ref, far_ref, *out_refs):
    for flip, out_ref in enumerate(out_refs):
        out_ref[0] = near_ref[flip]
        out_ref[1] = far_ref[flip]


def attend(got_ref, own_ref, a_ref, b_ref, c_ref, out_ref, top_ref, total_ref, sum_ref):
    queries = jnp.concatenate([got_ref[z] for z in range(Z)], axis=0)
    top_ref[...] = jnp.full((8, L), masked_score, f32)
    total_ref[...] = jnp.zeros((8, L), f32)
    sum_ref[...] = jnp.zeros((HS, L), f32)

    def one_block(doc_ref, b, carry):
        keys = doc_ref[b, :BLOCK, :]
        values = doc_ref[b, BLOCK : 2 * BLOCK, :]
        mask = doc_ref[b, 2 * BLOCK :, :].astype(f32)
        flags = jnp.concatenate([mask[0:8, :].T[:, :1], mask[0:8, :].T[:, 1:2]], axis=0)
        scores = jnp.dot(keys, queries, preferred_element_type=f32) * HS ** (-0.5)
        scores = jnp.where(flags > 0.5, scores, masked_score)
        highest = jnp.max(scores, axis=0, keepdims=True)
        weights = jnp.exp(scores - highest)
        total = jnp.sum(weights, axis=0, keepdims=True)
        weighted = lax.dot_general(
            values, weights.astype(bf16), (((0,), (0,)), ((), ())), preferred_element_type=f32
        )
        before = top_ref[0:1, :]
        ceiling = jnp.maximum(before, highest)
        old = jnp.exp(before - ceiling)
        new = jnp.exp(highest - ceiling)
        top_ref[0:1, :] = ceiling
        total_ref[0:1, :] = total_ref[0:1, :] * old + total * new
        sum_ref[...] = sum_ref[...] * old + weighted * new
        return carry

    for doc_ref in (own_ref, a_ref, b_ref, c_ref):
        lax.fori_loop(0, 2, functools.partial(one_block, doc_ref), 0)
    lane = lax.broadcasted_iota(jnp.int32, (1, 128), 1)
    for k in range(4):
        lanes = slice(k * 128, (k + 1) * 128)

        def fold(first, second, z):
            first, second = (
                (first, pltpu.roll(second, 64, 1)) if z == 0 else (pltpu.roll(first, 64, 1), second)
            )
            return jnp.where(lane < 64, first, second)

        upper = sum_ref[:64, lanes]
        lower = sum_ref[64:, lanes]
        top = top_ref[:, lanes]
        total = total_ref[:, lanes]
        row = lax.broadcasted_iota(jnp.int32, (8, 128), 0)
        for z in range(2):
            out_ref[2 * k + z, :64, :] = fold(upper, lower, z)
            tops = fold(top, top, z)
            totals = fold(total, total, z)
            out_ref[2 * k + z, 64:72, :] = jnp.where(
                row == 0, tops, jnp.where(row == 1, pltpu.roll(totals, 1, 0), 0.0)
            )


def join_blocks(got_ref, out_ref):
    ceiling = got_ref[0, 64:65, :]
    for z in range(1, Z):
        ceiling = jnp.maximum(ceiling, got_ref[z, 64:65, :])
    total = jnp.zeros((1, 128), f32)
    summed = jnp.zeros((64, 128), f32)
    for z in range(Z):
        factor = jnp.exp(got_ref[z, 64:65, :] - ceiling)
        total = total + got_ref[z, 65:66, :] * factor
        summed = summed + got_ref[z, :64, :] * factor
    folded = (summed / total).T
    attended = jnp.concatenate([folded[:64, :], folded[64:, :]], axis=1).astype(bf16)
    for g in range(G):
        out_ref[g] = attended


def output_part(got_ref, *refs):
    weights, out_ref = refs[:Z], refs[Z]
    attended = jnp.concatenate([got_ref[g] for g in range(G)], axis=1)
    for k in range(4):
        pair = jnp.concatenate([weights[2 * k][...], weights[2 * k + 1][...]], axis=0)
        out_ref[:, k * 128 : (k + 1) * 128] = lax.dot_general(
            attended, pair, (((1,), (1,)), ((), ())), preferred_element_type=f32
        )


def up_part(latents_ref, gain_ref, a_ref, b_ref, c_ref, d_ref, *refs):
    weights, out_ref, update_ref = refs[:Z], refs[Z], refs[Z + 1]
    update = (a_ref[...] + b_ref[...]) + (c_ref[...] + d_ref[...])
    state = latents_ref[...] + update
    gain = gain_ref[...]
    update_ref[...] = update
    squares = jnp.sum(state * state, axis=1, keepdims=True)
    scaled = (state * gain).astype(bf16)
    weight = jnp.concatenate([w[:64, :] for w in weights], axis=0)
    summed = jnp.dot(scaled, weight, preferred_element_type=f32)
    for g in range(G):
        rows = slice(g * 8, (g + 1) * 8)
        out_ref[g, :, :1024] = summed[rows, :]
        out_ref[g, :, 1024:] = jnp.broadcast_to(squares[rows, :], (8, 128))


def finish_hidden(got_ref, out_ref):
    summed = got_ref[0]
    for g in range(1, G):
        summed = summed + got_ref[g]
    inverse = lax.rsqrt(summed[:, 1024:1025] / D + epsilon)
    hidden = jax.nn.gelu(summed[:, :1024] * inverse).astype(bf16)
    for g in range(G):
        out_ref[g] = hidden


def down_part(place_ref, got_ref, update_ref, *refs):
    weights, out_ref = refs[:Z], refs[Z]
    hidden = jnp.concatenate([got_ref[g].astype(f32) for g in range(G)], axis=0).astype(bf16)
    for k in range(4):
        pair = jnp.concatenate([weights[2 * k][64:, :], weights[2 * k + 1][64:, :]], axis=0)
        lanes = slice(k * 128, (k + 1) * 128)
        summed = lax.dot_general(
            hidden, pair, (((1,), (1,)), ((), ())), preferred_element_type=f32
        )
        summed = summed + jnp.where(place_ref[3] == 0, update_ref[:, lanes], 0.0)
        turned = summed.T
        for half in range(2):
            z = lax.rem(place_ref[0] + RING[2 * k + half] + Z, Z)
            piece = turned[half * 64 : half * 64 + 64, :]
            folded = jnp.concatenate([piece[:32, :], piece[32:, :]], axis=1).astype(bf16)
            for x in range(4):
                out_ref[z * 4 + x] = folded


def unpack_encoded(lat_ref, got_ref, out_ref):
    lane = lax.broadcasted_iota(jnp.int32, (1, 128), 1)

    def summed(z):
        parts = [got_ref[4 * z + x].astype(f32) for x in range(4)]
        return (parts[0] + parts[1]) + (parts[2] + parts[3])

    for k in range(4):
        lanes = slice(k * 128, (k + 1) * 128)
        first, second = summed(2 * k), summed(2 * k + 1)
        out_ref[:32, lanes] = lat_ref[:32, lanes] + jnp.where(
            lane < 64, first, pltpu.roll(second, 64, 1)
        )
        out_ref[32:, lanes] = lat_ref[32:, lanes] + jnp.where(
            lane < 64, pltpu.roll(first, 64, 1), second
        )


def shifted(array, axis, step):
    count = lax.axis_size(axis)
    return lax.ppermute(array, axis, [(i, (i + step) % count) for i in range(count)])


def paired(array, axis, flip):
    return lax.ppermute(array, axis, [(i, i ^ flip) for i in range(lax.axis_size(axis))])


def together(*arrays):
    return lax.optimization_barrier(arrays)


class Ring:
    def __init__(self, array):
        self.forward, self.backward = [array], [array]

    def step(self):
        self.forward.append(shifted(self.forward[-1], "z", 1))
        if len(self.backward) < 4:
            self.backward.append(shifted(self.backward[-1], "z", -1))

    def tie(self, *others):
        held = together(*others, self.forward[-1], self.backward[-1])
        *others, self.forward[-1], self.backward[-1] = held
        return others[0] if len(others) == 1 else others

    def blocks(self):
        return self.forward + self.backward[1:]


def shards(
    latents,
    doc_keys,
    doc_values,
    token_mask,
    shard_lengths,
    query_weight,
    output_weight,
    attn_gain,
    up_weight,
    down_weight,
    mlp_gain,
):
    place = jnp.stack([lax.axis_index(name) for name in ("z", "y", "c", "x")]).astype(jnp.int32)
    attn_gain = attn_gain.reshape(1, 64)
    mlp_gain = mlp_gain.reshape(1, 64)
    latents = latents.T

    near = call(
        pack_projection,
        (shape((112, L), bf16),) * 4,
        4_000_000,
        (place, latents, attn_gain, query_weight),
        scalars=1,
    )
    start = near[0]
    near = [near[0]] + [paired(near[flip], "y", flip) for flip in (1, 2, 3)]
    crossed = [paired(piece, "c", 1) for piece in near]
    output_weight, mlp_weights, _ = together(
        output_weight.T, jnp.concatenate([up_weight, down_weight.T], axis=0), start
    )
    output_ring, mlp_ring = Ring(output_weight), Ring(mlp_weights)
    output_ring.step()
    crossed[0] = output_ring.tie(crossed[0])
    part = call(
        project_part, shape((Z, 104, 128), f32), 70_000_000, (*near, *crossed, latents, mlp_gain)
    )
    first = exchange(part, "z")
    half = shape((4, 2 * BLOCK + 16, HS), bf16)
    near_document, far_document = call(
        pack_document,
        (half, half),
        4_000_000,
        (shard_lengths, place, doc_keys, doc_values, token_mask.reshape(2, 128)),
        scalars=2,
        after=(part,),
    )
    far_document = paired(far_document, "c", 1)
    document = call(
        pair_document,
        (shape((2, 2 * BLOCK + 16, HS), bf16),) * 4,
        1_000_000,
        (near_document, far_document),
        after=(part,),
    )
    crossing = [document[0]]
    for flip in (1, 2, 3):
        crossing.append(paired(document[flip], "y", flip))
    document = crossing
    output_ring.step()
    first = output_ring.tie(first)
    queries = call(finish_queries, shape((Z, 16, L), bf16), 1_000_000, (first,))
    output_ring.step()
    mlp_ring.step()
    queries = exchange(queries, "z")
    queries = output_ring.tie(queries)
    output_ring.step()
    latent_rows, gain_row = call(
        place_latents,
        (shape((64, 512), f32), shape((1, 512), f32)),
        1_000_000,
        (place, first),
        scalars=1,
    )
    blocks = call(
        attend,
        shape((Z, 72, 128), f32),
        540_000_000,
        (queries, *document),
        scratch=(
            pltpu.VMEM((8, L), f32),
            pltpu.VMEM((8, L), f32),
            pltpu.VMEM((HS, L), f32),
        ),
    )
    blocks = output_ring.tie(blocks)
    blocks = mlp_ring.tie(blocks)
    mlp_ring.step()
    blocks = exchange(blocks, "z")
    blocks = mlp_ring.tie(blocks)
    attended = call(join_blocks, shape((G, 64, 128), bf16), 1_000_000, (blocks,))
    mlp_ring.step()
    attended = exchange(attended, YC)
    attended = mlp_ring.tie(attended)
    part = call(output_part, shape((64, 512), f32), 70_000_000, (attended, *output_ring.blocks()))
    parts = [part] + [paired(part, "x", flip) for flip in (1, 2, 3)]
    mlp_ring.step()
    weights = mlp_ring.blocks()
    summed, update = call(
        up_part,
        (shape((G, 8, 1152), f32), shape((64, 512), f32)),
        70_000_000,
        (latent_rows, gain_row, *parts, *weights),
    )
    summed = exchange(summed, YC)
    hidden = call(finish_hidden, shape((G, 8, 1024), bf16), 1_000_000, (summed,))
    hidden = exchange(hidden, YC)
    encoded = call(
        down_part,
        shape((32, 32, 128), bf16),
        70_000_000,
        (place, hidden, update, *weights),
        scalars=1,
    )
    encoded = exchange(encoded, ("z", "x"))
    return call(unpack_encoded, shape((64, L), f32), 1_000_000, (latents, encoded)).T


def solution(mesh):
    split = Mesh(mesh.devices.reshape(4, 8, 2, 4), ("y", "z", "c", "x"))
    return jax.shard_map(
        shards,
        mesh=split,
        in_specs=(
            P(None, TOK),
            P(TOK, "x"),
            P(TOK, "x"),
            P(TOK),
            P(TOK),
            P(TOK, "x"),
            P("x", TOK),
            P(TOK),
            P(TOK, "x"),
            P("x", TOK),
            P(TOK),
        ),
        out_specs=P(None, TOK),
        check_vma=False,
    )
```
